128 devices in a mesh: grp: 4 (over x, y), fiber: 16 (over z), tm: 2 (over core).
Axes of the slice: x: 2, y: 2, z: 16, core: 2. Of those that a mesh axis runs over, the one named last changes fastest.
The devices are a block of a 8x8x16 slice.
Arguments:
- samples: bfloat16 [64, 20480, 128], P('tm', ('grp', 'fiber')), parts along dimension 1, may hold values from -6 to 6
- counts: int32 [64], P(('grp', 'fiber')), parts along dimension 0, may hold values from 80 to 320
- reach_limit: int32 [20480], P(('grp', 'fiber')), parts along dimension 0, may hold values from 320 to 960
Outputs:
- coherence_real: bfloat16 [32, 20480, 960], P('tm', ('grp', 'fiber')), parts along dimension 1
- coherence_imag: bfloat16 [32, 20480, 960], P('tm', ('grp', 'fiber')), parts along dimension 1
The draws below stay inside these ranges and needn't reach their ends.
There are 4 independent parts, one for each index of `grp`. The reference program is written for one: setup_inputs(seed, part) draws one part's arguments, and reference() takes and returns one part's arrays. A program takes and returns all parts, laid end to end along the dimension named above; each array names one. Nothing has to cross between parts.
All inputs are finite; a program needn't handle non-finite values.
Results may differ from the reference program's by a relative error of at most 0.0069.
Values may be sent and summed in bfloat16 or wider, within the bound.
A program may use at most 576 MiB of HBM per device.

```python
import math
import jax
import jax.numpy as jnp
from jax import lax

FREQS = 32
SAMPLES = 128
FIRST_BIN = 8
CB = 320
WINDOWS = 64
CHANNELS = 5120
N_FIBER = 16


def place_ends(entries, rng, smallest, high):
    spot = [jax.random.randint(jax.random.fold_in(rng, axis), (), 0, length) for axis, length in enumerate(entries.shape)]
    widest = entries.shape.index(max(entries.shape))
    beside = spot[:widest] + [(spot[widest] + 1) % entries.shape[widest]] + spot[widest + 1:]
    return entries.at[tuple(spot)].set(smallest).at[tuple(beside)].set(high)


def block_scale(key, extent, pieces, least, top_value):
    loudness = 1.0
    for axis_at, blocks in pieces:
        draws = jax.random.uniform(jax.random.fold_in(jax.random.fold_in(key, 6), axis_at), (blocks,), jnp.float32, least / len(pieces), top_value / len(pieces))
        loudness = loudness * jnp.repeat(jnp.exp(draws), extent[axis_at] // blocks).reshape((-1,) + (1,) * (len(extent) - 1 - axis_at))
    return loudness


def bell_draw(own_key, extent, width, most, split=(), kind=jnp.bfloat16):
    factor_of = block_scale(own_key, extent, split, -0.22, 0.18) if split else 1.0
    values = jax.random.normal(own_key, extent, jnp.float32) * width * factor_of
    return jnp.minimum(jnp.maximum(values, -most), most).astype(kind)


def setup_inputs(seed: int = 0, part: int = 0) -> dict:
    seeds = jax.random.split(jax.random.key(seed), 4)
    part_keys = jax.random.split(jax.random.fold_in(seeds[3], part), 4)
    return {
        "samples": bell_draw(part_keys[0], (WINDOWS, CHANNELS, SAMPLES), 1.0, 6.0, ((0, 2), (1, 16))),
        "counts": place_ends(jax.random.randint(part_keys[1], (N_FIBER,), CB // 4, CB + 1), jax.random.fold_in(part_keys[1], 1), CB // 4, CB).astype(jnp.int32),
        "reach_limit": place_ends(jax.random.randint(part_keys[2], (CHANNELS,), CB, 3 * CB + 1), jax.random.fold_in(part_keys[2], 1), CB, 3 * CB).astype(jnp.int32),
    }


def make_table(length, bins, first_bin):
    steps_index = jnp.arange(length, dtype=jnp.int32)
    bin_index = jnp.arange(bins, dtype=jnp.int32) + first_bin
    products = steps_index[:, None] * bin_index[None, :] % length
    phases = 2.0 * math.pi * products.astype(jnp.float32) / length
    taper = 0.5 - 0.5 * jnp.cos(2.0 * math.pi * steps_index.astype(jnp.float32) / length)
    cosines = taper[:, None] * jnp.cos(phases)
    sines = -taper[:, None] * jnp.sin(phases)
    return jnp.concatenate([cosines, sines], axis=1).astype(jnp.bfloat16)

def diagonal_band(matrix):
    bins_here, rows, columns = matrix.shape
    flattened = matrix.reshape(bins_here, rows * columns)
    flattened = jnp.pad(flattened, ((0, 0), (0, rows)))
    return flattened.reshape(bins_here, rows, columns + 1)[:, :, 1:columns - rows + 1]

def reference(samples, counts, reach_limit):
    dft_table = make_table(SAMPLES, FREQS, FIRST_BIN)
    raw_spectra = jnp.einsum('wcl,lg->gwc', samples.astype(jnp.float32), dft_table.astype(jnp.float32))
    real_raw = raw_spectra[:FREQS]
    imag_raw = raw_spectra[FREQS:]
    level = lax.optimization_barrier(jnp.mean(real_raw * real_raw + imag_raw * imag_raw, axis=0))
    scale = lax.rsqrt(level + 1e-06)
    channel = jnp.arange(CHANNELS, dtype=jnp.int32)
    active = (channel % CB < counts[channel // CB]).astype(jnp.float32)
    real_part = (real_raw * scale * active).astype(jnp.bfloat16)
    imag_part = (imag_raw * scale * active).astype(jnp.bfloat16)
    real_wide = jnp.pad(real_part, ((0, 0), (0, 0), (0, 3 * CB))).astype(jnp.float32)
    imag_wide = jnp.pad(imag_part, ((0, 0), (0, 0), (0, 3 * CB))).astype(jnp.float32)
    power_sum = lax.optimization_barrier(jnp.sum(real_wide * real_wide + imag_wide * imag_wide, axis=1))
    inverse_root = lax.rsqrt(power_sum / WINDOWS + 1e-06)

    def per_block(block_index):
        start = (block_index * CB).astype(jnp.int32)
        left_real = lax.dynamic_slice_in_dim(real_wide, start, CB, 2)
        left_imag = lax.dynamic_slice_in_dim(imag_wide, start, CB, 2)
        right_real = lax.dynamic_slice_in_dim(real_wide, start, 4 * CB, 2)
        right_imag = lax.dynamic_slice_in_dim(imag_wide, start, 4 * CB, 2)
        cross_real = jnp.einsum('fwc,fwj->fcj', left_real, right_real) + jnp.einsum('fwc,fwj->fcj', left_imag, right_imag)
        cross_imag = jnp.einsum('fwc,fwj->fcj', left_imag, right_real) - jnp.einsum('fwc,fwj->fcj', left_real, right_imag)
        band_real = diagonal_band(cross_real)
        band_imag = diagonal_band(cross_imag)
        roots_right = lax.dynamic_slice_in_dim(inverse_root, start, 4 * CB, 1)
        own_scale = roots_right[:, :CB]
        partner = diagonal_band(jnp.broadcast_to(roots_right[:, None, :], (FREQS, CB, 4 * CB)))
        limits = lax.dynamic_slice_in_dim(reach_limit, start, CB, 0)
        offsets = jnp.arange(1, 3 * CB + 1, dtype=jnp.int32)
        in_reach = (offsets[None, :] <= limits[:, None]).astype(jnp.float32)
        factor = own_scale[:, :, None] * partner * in_reach[None, :, :] / math.sqrt(WINDOWS)
        return ((band_real * factor).astype(jnp.bfloat16), (band_imag * factor).astype(jnp.bfloat16))
    outputs = lax.map(per_block, jnp.arange(CHANNELS // CB, dtype=jnp.int32))
    coherence_real = outputs[0].transpose(1, 0, 2, 3).reshape(FREQS, CHANNELS, 3 * CB)
    coherence_imag = outputs[1].transpose(1, 0, 2, 3).reshape(FREQS, CHANNELS, 3 * CB)
    return (coherence_real, coherence_imag)
```

```python
import functools
import math

import jax
import jax.numpy as jnp
from jax import lax
from jax.experimental import pallas as pl
from jax.experimental.pallas import tpu as pltpu
from jax.sharding import PartitionSpec as P


FREQS = 32
FIRST_BIN = 8

LANE = 128
SUB = 8
PAIR = (((1,), (1,)), ((), ()))
PLAIN = (((1,), (0,)), ((), ()))


def sum_pieces(x):
    square = x * x
    upper = square.astype(jnp.bfloat16)
    lower = (square - upper.astype(jnp.float32)).astype(jnp.bfloat16)
    return upper, lower


def band_kernel(n_blocks, first, total_windows, tile0, per, *refs):
    bins_here = refs[0].shape[0]

    def one(b, carry):
        band_bin(b, n_blocks, first, total_windows, tile0, per, *refs)
        return carry

    lax.fori_loop(0, bins_here, one, 0)


def band_bin(b, n_blocks, first, total_windows, tile0, per, *refs):
    left_ref, reach_ref = refs[:2]
    blocks = refs[2:2 + n_blocks]
    out_re, out_im, both, right, cols, rows_s = refs[-6:]
    rows = left_ref.shape[1]
    quarter = LANE // 4
    lo = tile0
    hi = min(tile0 + per + 3, 11)

    wide = left_ref[b].astype(jnp.float32)
    back = (SUB - 1) - lax.broadcasted_iota(jnp.int32, (SUB, LANE), 0)
    wide = jnp.concatenate([jnp.take_along_axis(wide[i:i + SUB], back, axis=0) for i in range(0, rows, SUB)], axis=0)
    lane = lax.broadcasted_iota(jnp.int32, wide.shape, 1)
    odd = (lane // quarter) % 2 == 1
    swapped = jnp.where(odd, -pltpu.roll(wide, quarter, 1), pltpu.roll(wide, LANE - quarter, 1))
    upper, lower = sum_pieces(wide)
    ones = jnp.ones((LANE, LANE), jnp.bfloat16)
    power = lax.dot_general(upper, ones, PLAIN, preferred_element_type=jnp.float32) + lax.dot_general(lower, ones, PLAIN, preferred_element_type=jnp.float32)
    rows_s[...] = lax.rsqrt(power / total_windows + 1e-6) / math.sqrt(total_windows)
    for g in range(0, rows, LANE):
        count = min(LANE, rows - g)
        both[2 * g:2 * g + count, :] = wide[g:g + count].astype(jnp.bfloat16)
        both[2 * g + count:2 * g + 2 * count, :] = swapped[g:g + count].astype(jnp.bfloat16)
    ones = jnp.ones((SUB, LANE), jnp.bfloat16)
    values = [block[b] for block in blocks]
    if first + n_blocks == 4:
        values.append(jnp.zeros((11 * LANE - 4 * rows, LANE), jnp.bfloat16))
    joined = jnp.concatenate(values, axis=0)
    for v in range(lo, hi):
        at = v * LANE - first * rows
        piece = joined[at:at + LANE]
        upper, lower = sum_pieces(piece.astype(jnp.float32))
        right[:, v * LANE:(v + 1) * LANE] = piece.T
        power = lax.dot_general(ones, upper, PAIR, preferred_element_type=jnp.float32) + lax.dot_general(ones, lower, PAIR, preferred_element_type=jnp.float32)
        cols[:, v * LANE:(v + 1) * LANE] = lax.rsqrt(power / total_windows + 1e-6)

    lane = lax.broadcasted_iota(jnp.int32, (SUB, LANE), 1)
    for part in range(per):
        tile = tile0 + part
        for g in range(0, rows, LANE):
            count = min(LANE, rows - g)
            start = g + tile * LANE
            m = lax.dot_general(both[2 * g:2 * g + 2 * count, :], right[:, start:start + 2 * LANE], PLAIN, preferred_element_type=jnp.float32)
            c0 = cols[:, start:start + LANE]
            c1 = cols[:, start + LANE:start + 2 * LANE]
            turn = []
            for i in range(0, count, SUB):
                row = back + i
                take = lane > row
                offset = jnp.where(take, lane, lane + LANE) - row + tile * LANE
                at = g + i
                factor = jnp.where(offset <= reach_ref[at:at + SUB, :], jnp.where(take, c0, c1) * rows_s[at:at + SUB, :], 0.0)
                for shift in (0, count):
                    a = m[shift + i:shift + i + SUB]
                    z = jnp.where(take, a[:, :LANE], a[:, LANE:]) * factor
                    y = pltpu.roll(z, (2 * LANE - SUB - i) % LANE, 1, stride=1, stride_axis=0)
                    turn.append(jnp.take_along_axis(y, back, axis=0))
            for which, out in enumerate((out_re, out_im)):
                out[b, g:g + count, part * LANE:(part + 1) * LANE] = jnp.concatenate(turn[which::2], axis=0).astype(jnp.bfloat16)


def band_call(left, reach, blocks, first, width, place, bin0, nb, step, outs, total_windows):
    rows, depth = left.shape[1:]
    n = len(blocks)
    bins = left.shape[0]
    in_specs = [pl.BlockSpec((step, rows, depth), lambda f: (bin0 // step + f, 0, 0)),
                pl.BlockSpec((rows, LANE), lambda f: (0, 0))]
    args = [left, reach]
    for arr, off in blocks:
        in_specs.append(pl.BlockSpec((step, rows, depth), functools.partial(lambda off, f: (off + f, 0, 0), off // step)))
        args.append(arr)
    alias = {}
    if outs is not None:
        for i, o in enumerate(outs):
            alias[len(args)] = i
            in_specs.append(pl.BlockSpec(memory_space=pl.ANY))
            args.append(o)
    out_shape = [jax.ShapeDtypeStruct((bins, rows, 3 * rows), jnp.bfloat16)] * 2
    out_specs = [pl.BlockSpec((step, rows, width), lambda f: (bin0 // step + f, 0, place))] * 2
    per = min(width, 8 * LANE - place * width) // LANE
    return pl.pallas_call(
        functools.partial(band_kernel, n, first, float(total_windows), place * width // LANE, per),
        grid=(nb // step,), in_specs=in_specs, out_specs=out_specs, out_shape=out_shape,
        input_output_aliases=alias,
        scratch_shapes=[pltpu.VMEM((2 * rows, depth), jnp.bfloat16), pltpu.VMEM((depth, 11 * LANE), jnp.bfloat16),
                        pltpu.VMEM((SUB, 11 * LANE), jnp.float32), pltpu.VMEM((rows, LANE), jnp.float32)],
        compiler_params=pltpu.CompilerParams(dimension_semantics=("arbitrary",)),
        cost_estimate=pl.CostEstimate(flops=nb * per * 300_000_000, bytes_accessed=nb * rows * width * 4, transcendentals=0),
    )(*args)


def make_table(length, bins, first_bin):
    steps_index = jnp.arange(length, dtype=jnp.int32)
    bin_index = jnp.arange(bins, dtype=jnp.int32) + first_bin
    products = steps_index[:, None] * bin_index[None, :] % length
    phases = 2.0 * math.pi * products.astype(jnp.float32) / length
    taper = 0.5 - 0.5 * jnp.cos(2.0 * math.pi * steps_index.astype(jnp.float32) / length)
    cosines = taper[:, None] * jnp.cos(phases)
    sines = -taper[:, None] * jnp.sin(phases)
    return jnp.concatenate([cosines, sines], axis=1).astype(jnp.bfloat16)


def own_spectra(samples, counts):
    windows, width = samples.shape[:2]
    table = make_table(samples.shape[2], FREQS, FIRST_BIN)
    raw = jnp.einsum("wcl,lg->gwc", samples, table, preferred_element_type=jnp.float32)
    real_raw, imag_raw = raw[:FREQS], raw[FREQS:]
    level = jnp.mean(real_raw * real_raw + imag_raw * imag_raw, axis=0)
    active = (lax.iota(jnp.int32, width) < counts[0]).astype(jnp.float32)
    scale = lax.rsqrt(level + 1e-06)
    parts = jnp.stack([real_raw, imag_raw], axis=1) * scale * active
    parts = parts.astype(jnp.bfloat16).reshape(FREQS, 2 * windows, width)
    return parts.transpose(0, 2, 1)


def body(samples, counts, reach_limit):
    rows = samples.shape[1]
    total_windows = samples.shape[0] * lax.axis_size("tm")
    mine = own_spectra(samples, counts)
    own = lax.all_to_all(mine, "tm", split_axis=0, concat_axis=2, tiled=True)
    devices = lax.axis_size("fiber")
    route = [(i, i - 1) for i in range(1, devices)]
    reach = jnp.broadcast_to(reach_limit.reshape(-1, SUB)[:, ::-1].reshape(-1, 1), (rows, LANE))
    spans = []
    at = 0
    for size in CHUNKS:
        spans.append((at, size))
        at += size
    held = [[(own, at) for at, size in spans]]
    for distance in range(3):
        if distance == 0:
            pieces = [own[at:at + size] for at, size in spans]
        else:
            pieces = [piece for piece, _ in held[-1]]
        moved = []
        for piece in pieces:
            moved.append((lax.ppermute(piece, "fiber", route), 0))
        held.append(moved)
    outs = None
    for first, last, width, place in ((0, 1, 256, 0), (0, 2, 256, 1), (1, 3, 512, 1)):
        for i, (at, size) in enumerate(spans):
            blocks = [held[d][i] for d in range(first, last + 1)]
            outs = band_call(own, reach, blocks, first, width, place, at, size, STEP, outs, total_windows)
    return tuple(outs)


CHUNKS = (10, 6)
STEP = 2


def solution(mesh):
    placed = (P("tm", ("grp", "fiber"), None), P(("grp", "fiber")), P(("grp", "fiber")))
    return jax.shard_map(
        body,
        mesh=mesh,
        in_specs=placed,
        out_specs=(P("tm", ("grp", "fiber"), None), P("tm", ("grp", "fiber"), None)),
        check_vma=False,
    )
```

```python
import functools
import math

import jax
import jax.numpy as jnp
import numpy as np
from jax import lax
from jax.experimental import pallas as pl
from jax.experimental.pallas import tpu as pltpu
from jax.sharding import PartitionSpec as P


FREQS = 32
FIRST_BIN = 8
LANE = 128
SUB = 8
PITCH = LANE + SUB
SPECTRA_STEP = 8
SPANS = ((0, 8), (8, 4), (12, 4))
STEP = 2
PAIR = (((1,), (1,)), ((), ()))
PLAIN = (((1,), (0,)), ((), ()))


def make_table(length, bins, first_bin):
    steps = np.arange(length)
    products = (steps[None, :] * (np.arange(bins) + first_bin)[:, None]) % length
    phases = (2.0 * math.pi * products / length).astype(np.float32)
    taper = (0.5 - 0.5 * np.cos((2.0 * math.pi * steps / length).astype(np.float32))).astype(np.float32)
    table = np.concatenate([taper * np.cos(phases), -taper * np.sin(phases)], axis=0)
    return jnp.asarray(table.astype(np.float32), jnp.bfloat16)


def spectra_kernel(spans, samples_ref, table_ref, counts_ref, *refs):
    outs = refs[:len(spans)]
    gathered, mine, theirs, send_sem, recv_sem = refs[len(spans):]
    step = pl.program_id(0)
    here = samples_ref.shape[0]
    bins = table_ref.shape[0] // 4
    side = lax.axis_index("tm")

    def transfer(f):
        return pltpu.make_async_remote_copy(
            src_ref=mine.at[f], dst_ref=theirs.at[f], send_sem=send_sem.at[f], recv_sem=recv_sem.at[f],
            device_id={"tm": 1 - side}, device_id_type=pl.DeviceIdType.MESH)

    @pl.when(step == 0)
    def _():
        barrier = pltpu.get_barrier_semaphore()
        pl.semaphore_signal(barrier, inc=1, device_id={"tm": 1 - side}, device_id_type=pl.DeviceIdType.MESH)
        pl.semaphore_wait(barrier, 1)

    width = samples_ref.shape[1]
    tiles = pl.cdiv(width, LANE)
    active = (lax.broadcasted_iota(jnp.int32, (1, width), 1) < counts_ref[0]).astype(jnp.float32)
    for i in range(here):
        raw = lax.dot_general(table_ref[...], samples_ref[i], PAIR, preferred_element_type=jnp.float32)
        level = jnp.sum(raw * raw, axis=0, keepdims=True) * (1.0 / (2 * bins))
        value = raw * (lax.rsqrt(level + 1e-6) * active)
        for part in range(2):
            for half in range(2):
                row = half * (LANE // 2) + part * (LANE // 4) + step * here + i
                at = (2 * part + half) * bins
                for k in range(tiles):
                    piece = value[at:at + bins, k * LANE:min(width, (k + 1) * LANE)]
                    if piece.shape[1] < LANE:
                        piece = jnp.concatenate([piece, jnp.zeros((bins, LANE - piece.shape[1]), jnp.float32)], axis=1)
                    gathered[pl.ds(k * bins * PITCH + row, bins, stride=PITCH), :] = piece

    @pl.when(step == pl.num_programs(0) - 1)
    def _():
        def turn(f, carry):
            for k in range(tiles):
                tile = gathered[pl.ds(pl.multiple_of((k * bins + f) * PITCH, SUB), LANE), :]
                near = slice(k * LANE, min(width, (k + 1) * LANE))
                mine[f, near] = tile.astype(jnp.bfloat16).T[:near.stop - near.start]

            @pl.when(f > 0)
            def _():
                transfer(f - 1).start()

            return carry

        lax.fori_loop(0, bins, turn, 0)
        transfer(bins - 1).start()
        lane = lax.broadcasted_iota(jnp.int32, mine.shape[1:], 1)
        for out, (at, size) in zip(outs, spans):
            def merge(i, carry):
                f = at + i
                transfer(f).wait_recv()
                other = pltpu.roll(theirs[f].astype(jnp.float32), LANE // 2, 1)
                out[i] = jnp.where(lane // (LANE // 2) == side, mine[f].astype(jnp.float32), other).astype(jnp.bfloat16)
                return carry

            lax.fori_loop(0, size, merge, 0)

        def finish(f, carry):
            transfer(f).wait_send()
            return carry

        lax.fori_loop(0, bins, finish, 0)


def own_spectra(samples, counts, spans):
    windows, width, length = samples.shape
    bins = FREQS // 2
    here = SPECTRA_STEP
    table = make_table(length, FREQS, FIRST_BIN)
    block = lambda size: (size, width, LANE)
    return pl.pallas_call(
        functools.partial(spectra_kernel, spans),
        grid=(windows // here,),
        in_specs=[pl.BlockSpec((here, width, length), lambda s: (s, 0, 0)),
                  pl.BlockSpec((2 * FREQS, length), lambda s: (0, 0)),
                  pl.BlockSpec(memory_space=pltpu.SMEM)],
        out_specs=[pl.BlockSpec(block(size), lambda s: (0, 0, 0)) for _, size in spans],
        out_shape=[jax.ShapeDtypeStruct(block(size), jnp.bfloat16) for _, size in spans],
        scratch_shapes=[pltpu.VMEM((pl.cdiv(width, LANE) * bins * PITCH, LANE), jnp.float32),
                        pltpu.VMEM(block(bins), jnp.bfloat16), pltpu.VMEM(block(bins), jnp.bfloat16),
                        pltpu.SemaphoreType.DMA((bins,)), pltpu.SemaphoreType.DMA((bins,))],
        compiler_params=pltpu.CompilerParams(collective_id=0, has_side_effects=True, dimension_semantics=("arbitrary",)),
        cost_estimate=pl.CostEstimate(flops=3_000_000_000, bytes_accessed=5_000_000, transcendentals=0),
    )(samples, table, counts)


def sum_pieces(x):
    square = x * x
    upper = square.astype(jnp.bfloat16)
    lower = (square - upper.astype(jnp.float32)).astype(jnp.bfloat16)
    return upper, lower


def band_kernel(n_blocks, first, total_windows, tile0, per, *refs):
    bins_here = refs[0].shape[0]

    def one(b, carry):
        band_bin(b, n_blocks, first, total_windows, tile0, per, *refs)
        return carry

    lax.fori_loop(0, bins_here, one, 0)


def band_bin(b, n_blocks, first, total_windows, tile0, per, *refs):
    left_ref, reach_ref = refs[:2]
    blocks = refs[2:2 + n_blocks]
    out_re, out_im, both, right, cols, rows_s = refs[-6:]
    rows = left_ref.shape[1]
    quarter = LANE // 4
    lo = tile0
    hi = min(tile0 + per + 3, 11)

    wide = left_ref[b].astype(jnp.float32)
    back = (SUB - 1) - lax.broadcasted_iota(jnp.int32, (SUB, LANE), 0)
    wide = jnp.concatenate([jnp.take_along_axis(wide[i:i + SUB], back, axis=0) for i in range(0, rows, SUB)], axis=0)
    lane = lax.broadcasted_iota(jnp.int32, wide.shape, 1)
    odd = (lane // quarter) % 2 == 1
    swapped = jnp.where(odd, -pltpu.roll(wide, quarter, 1), pltpu.roll(wide, LANE - quarter, 1))
    upper, lower = sum_pieces(wide)
    ones = jnp.ones((LANE, LANE), jnp.bfloat16)
    power = lax.dot_general(upper, ones, PLAIN, preferred_element_type=jnp.float32) + lax.dot_general(lower, ones, PLAIN, preferred_element_type=jnp.float32)
    rows_s[...] = lax.rsqrt(power / total_windows + 1e-6) / math.sqrt(total_windows)
    for g in range(0, rows, LANE):
        count = min(LANE, rows - g)
        both[2 * g:2 * g + count, :] = wide[g:g + count].astype(jnp.bfloat16)
        both[2 * g + count:2 * g + 2 * count, :] = swapped[g:g + count].astype(jnp.bfloat16)
    ones = jnp.ones((SUB, LANE), jnp.bfloat16)
    values = [block[b] for block in blocks]
    if first + n_blocks == 4:
        values.append(jnp.zeros((11 * LANE - 4 * rows, LANE), jnp.bfloat16))
    joined = jnp.concatenate(values, axis=0)
    for v in range(lo, hi):
        at = v * LANE - first * rows
        piece = joined[at:at + LANE]
        upper, lower = sum_pieces(piece.astype(jnp.float32))
        right[:, v * LANE:(v + 1) * LANE] = piece.T
        power = lax.dot_general(ones, upper, PAIR, preferred_element_type=jnp.float32) + lax.dot_general(ones, lower, PAIR, preferred_element_type=jnp.float32)
        cols[:, v * LANE:(v + 1) * LANE] = lax.rsqrt(power / total_windows + 1e-6)

    lane = lax.broadcasted_iota(jnp.int32, (SUB, LANE), 1)
    for g in range(0, rows, LANE):
        count = min(LANE, rows - g)
        start = g + tile0 * LANE
        m = lax.dot_general(both[2 * g:2 * g + 2 * count, :], right[:, start:start + (per + 1) * LANE], PLAIN, preferred_element_type=jnp.float32)
        for part in range(per):
            tile = tile0 + part
            at = part * LANE
            c0 = cols[:, start + at:start + at + LANE]
            c1 = cols[:, start + at + LANE:start + at + 2 * LANE]
            turn = []
            for i in range(0, count, SUB):
                row = back + i
                take = lane > row
                offset = jnp.where(take, lane, lane + LANE) - row + tile * LANE
                near = slice(g + i, g + i + SUB)
                factor = jnp.where(offset <= reach_ref[near, :], jnp.where(take, c0, c1) * rows_s[near, :], 0.0)
                for shift in (0, count):
                    up = slice(shift + i, shift + i + SUB)
                    z = jnp.where(take, m[up, at:at + LANE], m[up, at + LANE:at + 2 * LANE]) * factor
                    y = pltpu.roll(z, (2 * LANE - SUB - i) % LANE, 1, stride=1, stride_axis=0)
                    turn.append(jnp.take_along_axis(y, back, axis=0))
            for which, out in enumerate((out_re, out_im)):
                wide = min(LANE, out.shape[2] - at)
                out[b, g:g + count, at:at + wide] = jnp.concatenate(turn[which::2], axis=0).astype(jnp.bfloat16)[:, :wide]


def band_call(bins, left, reach, blocks, first, width, place, bin0, step, outs, total_windows):
    nb, rows, depth = left.shape
    n = len(blocks)
    in_specs = [pl.BlockSpec((step, rows, depth), lambda f: (f, 0, 0)),
                pl.BlockSpec((rows, LANE), lambda f: (0, 0))]
    args = [left, reach]
    for block in blocks:
        in_specs.append(pl.BlockSpec((step, rows, depth), lambda f: (f, 0, 0)))
        args.append(block)
    alias = {}
    if outs is not None:
        for i, o in enumerate(outs):
            alias[len(args)] = i
            in_specs.append(pl.BlockSpec(memory_space=pl.ANY))
            args.append(o)
    out_shape = [jax.ShapeDtypeStruct((bins, rows, 3 * rows), jnp.bfloat16)] * 2
    out_specs = [pl.BlockSpec((step, rows, width), lambda f: (bin0 // step + f, 0, place))] * 2
    per = min(pl.cdiv(width, LANE), 8 - place * width // LANE)
    return pl.pallas_call(
        functools.partial(band_kernel, n, first, float(total_windows), place * width // LANE, per),
        grid=(nb // step,), in_specs=in_specs, out_specs=out_specs, out_shape=out_shape,
        input_output_aliases=alias,
        scratch_shapes=[pltpu.VMEM((2 * rows, depth), jnp.bfloat16), pltpu.VMEM((depth, 11 * LANE), jnp.bfloat16),
                        pltpu.VMEM((SUB, 11 * LANE), jnp.float32), pltpu.VMEM((rows, LANE), jnp.float32)],
        compiler_params=pltpu.CompilerParams(dimension_semantics=("arbitrary",), vmem_limit_bytes=16 * 1024 * 1024),
        cost_estimate=pl.CostEstimate(flops=nb * per * 300_000_000, bytes_accessed=nb * rows * width * 4, transcendentals=0),
    )(*args)


def body(samples, counts, reach_limit):
    rows = samples.shape[1]
    total_windows = samples.shape[0] * lax.axis_size("tm")
    own = own_spectra(samples, counts, SPANS)
    bins = SPANS[-1][0] + SPANS[-1][1]
    devices = lax.axis_size("fiber")
    down = [(i, i - 1) for i in range(1, devices)]
    held = [list(own)]
    for _ in range(3):
        moved = []
        for piece in held[-1]:
            moved.append(lax.ppermute(piece, "fiber", down))
        held.append(moved)
    reach = jnp.broadcast_to(reach_limit.reshape(-1, SUB)[:, ::-1].reshape(-1, 1), (rows, LANE))
    outs = None
    stages = ((0, 1, 256, 0), (0, 2, 256, 1), (1, 3, 512, 1))
    for low, high, width, place in stages:
        for i in range(len(SPANS)):
            blocks = [held[d][i] for d in range(low, high + 1)]
            outs = band_call(bins, own[i], reach, blocks, low, width, place, SPANS[i][0], STEP, outs, total_windows)
    return tuple(outs)


def solution(mesh):
    placed = (P("tm", ("grp", "fiber"), None), P(("grp", "fiber")), P(("grp", "fiber")))
    return jax.shard_map(
        body,
        mesh=mesh,
        in_specs=placed,
        out_specs=(P("tm", ("grp", "fiber"), None), P("tm", ("grp", "fiber"), None)),
        check_vma=False,
    )
```
